256 devices in a mesh: rows: 64 (over z, y, core), cols: 4 (over x).
Axes of the slice: x: 4, y: 4, z: 8, core: 2. Of those that a mesh axis runs over, the one named last changes fastest.
Arguments:
- factor: float32 [65536, 1024], P('rows', 'cols'), as said below
- right_side: float32 [65536, 1024], P('rows', 'cols'), may hold values from -6 to 6
- later_solution: float32 [65536, 1024], P('rows', 'cols'), may hold values from -6 to 6
Outputs:
- updated_side: float32 [65536, 1024], P('rows', 'cols')
- head_solution: float32 [1024, 1024], P(('cols', 'rows'))
The draws below stay inside these ranges and needn't reach their ends.
Inputs may be any that keep to these rules, and one draw needn't show every extreme that they name: `factor`: the first 1024 rows form a lower triangular matrix with diagonal entries between 0.25 and 1.1.
All inputs are finite; a program needn't handle non-finite values.
Results may differ from the reference program's by a relative error of at most 0.00018.
Values sent between devices are 32-bit elements; how exact they have to be, the bound alone decides.
No kernel may reach another device: no remote copies, remote signals or barrier semaphores. Data moves between devices by JAX's collectives and lax.ppermute only.
A program may use at most 64 MiB of HBM per device.

```python
import math
import jax
import jax.numpy as jnp
from jax import lax

WINDOW = 1024
FACTOR_ROWS = 65536
QUERIES = 1024


def draw_factor(key, part):
    key_normal, key_points = jax.random.split(key, 2)
    normal_part = jax.random.normal(key_normal, (FACTOR_ROWS, WINDOW), jnp.float32)
    row_index = jnp.arange(FACTOR_ROWS)[:, None]
    side_length = (WINDOW / 1024.0) ** (1.0 / 3.0)
    points = jax.random.uniform(key_points, (WINDOW, 3), jnp.float32, 0.0, side_length)
    length_scale = 0.1
    noise_level = 0.1
    row_scale = jnp.ones((FACTOR_ROWS, 1), jnp.float32)
    differences = points[:, None, :] - points[None, :, :]
    distances = jnp.sum(differences * differences, axis=-1)
    kernel = jnp.exp(-distances / (2.0 * length_scale * length_scale)) + noise_level * jnp.eye(WINDOW, dtype=jnp.float32)
    head_lower = jnp.tril(jnp.linalg.cholesky(kernel))
    head_padded = jnp.concatenate([head_lower, jnp.zeros((FACTOR_ROWS - WINDOW, WINDOW), jnp.float32)], axis=0)
    tail_part = 2.0 / math.sqrt(FACTOR_ROWS) * row_scale * normal_part
    return jnp.where(row_index < WINDOW, head_padded, tail_part)


def levels(rng, shape, shards, low, largest):
    gain = 1.0
    for dim, shards_of in shards:
        draws = jax.random.uniform(jax.random.fold_in(jax.random.fold_in(rng, 6), dim), (shards_of,), jnp.float32, low / len(shards), largest / len(shards))
        gain = gain * jnp.repeat(jnp.exp(draws), shape[dim] // shards_of).reshape((-1,) + (1,) * (len(shape) - 1 - dim))
    return gain


def noise(stream_key, extent, deviation, limit, cuts=(), held_as=jnp.bfloat16):
    entries = jax.random.normal(stream_key, extent, jnp.float32) * deviation
    if len(cuts) > 0:
        entries = levels(stream_key, extent, cuts, -0.22, 0.18) * entries
    return jnp.clip(entries, min=-limit, max=limit).astype(held_as)


def setup_inputs(seed: int = 0) -> dict:
    keys = jax.random.split(jax.random.key(seed), 4)
    return {
        "factor": draw_factor(jax.random.fold_in(keys[3], 71), 0),
        "right_side": noise(keys[1], (FACTOR_ROWS, QUERIES), 1.0, 6.0, ((0, 64), (1, 4)), jnp.float32),
        "later_solution": noise(keys[2], (FACTOR_ROWS, QUERIES), 1.0, 6.0, ((0, 64), (1, 4)), jnp.float32),
    }


def reference(factor, right_side, later_solution):
    precise = lax.Precision.HIGHEST
    head_block = factor[:WINDOW]
    tail_block = factor[WINDOW:]
    solved = lax.linalg.triangular_solve(head_block, right_side[:WINDOW], left_side=True, lower=True)
    product = jnp.dot(tail_block.astype(jnp.float32), solved.astype(jnp.float32), precision=precise, preferred_element_type=jnp.float32)
    updated_side = jnp.concatenate([solved, right_side[WINDOW:] - product], axis=0)
    later_rows = later_solution[WINDOW:]
    summed = lax.dot_general(later_rows.astype(jnp.float32), tail_block.astype(jnp.float32), (((0,), (0,)), ((), ())), precision=precise, preferred_element_type=jnp.float32)
    target = solved.T - summed
    head_solution = lax.linalg.triangular_solve(head_block, target, left_side=False, lower=True)
    return (updated_side, head_solution)
```

```python
import jax
import jax.numpy as jnp
from jax import lax
from jax.experimental import pallas as pl
from jax.experimental.pallas import tpu as pltpu
from jax.sharding import Mesh
from jax.sharding import PartitionSpec as P

WINDOW = 1024
ROW_AXES = ("z", "y", "c")
Z, Y, C, X = 8, 4, 2, 4
HIGHEST = lax.Precision.HIGHEST
HIGH = lax.Precision.HIGH


def dot(a,b): return jnp.dot(a,b,precision=HIGHEST,preferred_element_type=jnp.float32)
def inverse_kernel(l_ref, o_ref):
    row = lax.broadcasted_iota(jnp.int32,(256,256),0)
    lane = lax.broadcasted_iota(jnp.int32,(256,256),1)
    i32 = row[:32]; lane32 = lane[:32]; j32 = lane32 % 32
    full=[]
    packs=[]
    for g in range(4):
        p = jnp.zeros((32,256),jnp.float32)
        for b in range(8):
            p = jnp.where(lane32//32==b, l_ref[pl.ds(g*256+b*32,32),pl.ds(g*256,256)], p)
        packs.append(p)
    ds=[jnp.where(i32==j32, 1.0/p, 0.0) for p in packs]
    spread=lambda v: jnp.where(row//32==lane//32, jnp.concatenate([v]*8,axis=0), 0.0)
    for s in (1,2,4,8,16):
        m=(i32//(2*s)==j32//(2*s)) & (i32//s != j32//s) & (i32>j32)
        eds=[dot(jnp.where(m,p,0.0), spread(d)) for p,d in zip(packs,ds)]
        ds=[d-dot(d,spread(e)) for d,e in zip(ds,eds)]
    full=[spread(d) for d in ds]
    for n in (32,64,128):
        same=(row//(2*n))==(lane//(2*n))
        low=(row%(2*n))>=n
        left=(lane%(2*n))<n
        ln=lane[:n]
        reps=256//n
        new=[]
        bs=[]; cs=[]
        for g in range(4):
            bp=jnp.zeros((n,256),jnp.float32); cp=jnp.zeros((n,256),jnp.float32)
            for b in range(reps//2):
                here=ln//(2*n)==b
                bp=jnp.where(here & (ln%(2*n)<n), l_ref[pl.ds(g*256+b*2*n+n,n),pl.ds(g*256,256)], bp)
                cp=jnp.where(here & (ln%(2*n)>=n), full[g][b*2*n+n:b*2*n+2*n,:], cp)
            bs.append(bp); cs.append(cp)
        bas=[dot(bp,f) for bp,f in zip(bs,full)]
        rs=[dot(cp,jnp.where(same&low,jnp.concatenate([ba]*reps,axis=0),0.0)) for cp,ba in zip(cs,bas)]
        full=[f-jnp.where(same&low&left,jnp.concatenate([r]*reps,axis=0),0.0) for f,r in zip(full,rs)]
    blk=lambda i,j: l_ref[pl.ds(i*256,256),pl.ds(j*256,256)]
    def put(i,j,v): o_ref[pl.ds(i*256,256),pl.ds(j*256,256)]=v
    off=[]
    t=[dot(blk(2*p+1,2*p),full[2*p]) for p in range(2)]
    off=[-dot(full[2*p+1],t[p]) for p in range(2)]
    a00,a10,a11=full[0],off[0],full[1]
    c00,c10,c11=full[2],off[1],full[3]
    z=jnp.zeros((256,256),jnp.float32)
    put(0,0,a00);put(1,0,a10);put(1,1,a11);put(2,2,c00);put(3,2,c10);put(3,3,c11)
    put(0,1,z);put(0,2,z);put(0,3,z);put(1,2,z);put(1,3,z);put(2,3,z)
    b0=l_ref[pl.ds(512,512),pl.ds(0,256)]; b1=l_ref[pl.ds(512,512),pl.ds(256,256)]
    ba0=dot(b0,a00)+dot(b1,a10)
    ba1=dot(b1,a11)
    for j,ba in ((0,ba0),(1,ba1)):
        put(2,j,-dot(c00,ba[:256]))
        put(3,j,-(dot(c10,ba[:256])+dot(c11,ba[256:])))
def inverse(l, interpret=False):
    return pl.pallas_call(inverse_kernel,out_shape=jax.ShapeDtypeStruct((1024,1024),jnp.float32),
        in_specs=[pl.BlockSpec(memory_space=pltpu.VMEM)],out_specs=pl.BlockSpec(memory_space=pltpu.VMEM),
        compiler_params=pltpu.CompilerParams(vmem_limit_bytes=40*1024*1024),interpret=interpret)(l)


def shift(value, axis, by):
    size = lax.axis_size(axis)
    return lax.ppermute(value, axis, [(i, (i + by) % size) for i in range(size)])


def device(z, y, c):
    return (z * Y + y) * C + c


def tree_steps():
    orders = {
        0: [("z", 4), ("z", 2), ("z", 1), ("y", 2), ("y", 1)],
        1: [("y", 2), ("y", 1), ("z", 4), ("z", 2), ("z", 1)],
    }
    steps = []
    for t in range(5):
        pairs = []
        for core, order in orders.items():
            holders = [(0, 0)]
            for axis, d in order[:t]:
                holders += [(a + d, b) if axis == "z" else (a, b + d) for a, b in holders]
            axis, d = order[t]
            for a, b in holders:
                to = (a + d, b) if axis == "z" else (a, b + d)
                pairs.append((device(a, b, core), device(*to, core)))
        steps.append(pairs)
    return steps


TREE = tree_steps()


def spread_halves(array):
    half = array.shape[0] // 2
    core = lax.axis_index("c")
    me = lax.axis_index(ROW_AXES)
    other = lax.ppermute(array[half:], ROW_AXES, [(0, 1)])
    held = jnp.where(core == 0, array[:half], other)
    for pairs in TREE:
        got = lax.ppermute(held, ROW_AXES, pairs)
        table = [False] * (Z * Y * C)
        for _, to in pairs:
            table[to] = True
        held = jnp.where(jnp.asarray(table)[me], got, held)
    return held


def join_halves(half):
    core = lax.axis_index("c")
    other = shift(half, "c", 1)
    return jnp.concatenate(
        [jnp.where(core == 0, half, other), jnp.where(core == 0, other, half)], axis=0
    )


def gather_cols(own):
    half = own.shape[0] // 2
    left = shift(own, "x", 1)
    right = shift(own, "x", -1)
    top = shift(left[:half], "x", 1)
    bottom = shift(right[half:], "x", -1)
    return own, left, right, jnp.concatenate([top, bottom], axis=0)


def in_order(blocks):
    x = lax.axis_index("x")
    rows, width = blocks[0].shape
    out = jnp.zeros((rows, X * width), jnp.float32)
    for block, by in zip(blocks, (0, -1, 1, 2)):
        out = lax.dynamic_update_slice(out, block, (0, ((x + by) % X) * width))
    return out


def on_device(factor, right_side, later_solution):
    x = lax.axis_index("x")
    z, y, c = (lax.axis_index(a) for a in ROW_AXES)
    is_head = lax.axis_index(ROW_AXES) == 0
    factor_blocks = gather_cols(factor)
    lower_half = spread_halves(factor)
    solved_own = jnp.dot(
        inverse(in_order(factor_blocks)), right_side,
        precision=HIGHEST, preferred_element_type=jnp.float32,
    )
    later_rows = jnp.where(is_head, 0.0, later_solution)
    partial = [
        lax.dot_general(later_rows, f, (((0,), (0,)), ((), ())), precision=HIGH,
                        preferred_element_type=jnp.float32)
        for f in factor_blocks
    ]
    first = jnp.concatenate(partial[:2], axis=1)
    second = jnp.concatenate(partial[2:], axis=1)
    keep = jnp.where(c == 0, first, second)
    give = jnp.where(c == 0, second, first)
    part = keep + shift(give, "c", 1)
    part = part.reshape(2, 2, 2, 2, 2, 8, 512)
    for axis, index, bit, dim in (
        ("y", y, 1, 4), ("z", z, 1, 2), ("y", y, 2, 3), ("z", z, 2, 1), ("z", z, 4, 0)
    ):
        mine = (index // bit) % 2
        kept = lax.dynamic_slice_in_dim(part, mine, 1, dim)
        sent = lax.dynamic_slice_in_dim(part, 1 - mine, 1, dim)
        size = lax.axis_size(axis)
        part = kept + lax.ppermute(sent, axis, [(i, i ^ bit) for i in range(size)])
    part = part.reshape(8, 512)
    kept = lax.dynamic_slice_in_dim(part, 4 * c, 4, 0)
    sent = lax.dynamic_slice_in_dim(part, 4 * (1 - c), 4, 0)
    other = shift(sent, "c", 1)
    both = jnp.concatenate(
        [jnp.where(c == 0, kept, other), jnp.where(c == 0, other, kept)], axis=1
    )
    summed = in_order([both[:, 256 * i : 256 * (i + 1)] for i in range(X)])
    lower = join_halves(in_order(gather_cols(lower_half)))
    lower_inverse = inverse(lower)
    solved = join_halves(spread_halves(solved_own))
    product = 0.0
    for f, by in zip(factor_blocks, (0, -1, 1, 2)):
        rows = lax.dynamic_slice_in_dim(solved, ((x + by) % X) * 256, 256, 0)
        product = product + jnp.dot(f, rows, precision=HIGH, preferred_element_type=jnp.float32)
    updated_side = jnp.where(is_head, solved, right_side - product)
    share = lax.axis_index(ROW_AXES) * 4
    pick = (share + jnp.arange(4)[:, None] == jnp.arange(256)[None, :]).astype(jnp.float32)
    solved_share = lax.dot_general(
        pick, solved, (((1,), (1,)), ((), ())), precision=HIGHEST,
        preferred_element_type=jnp.float32,
    )
    head_solution = jnp.dot(
        solved_share - summed, lower_inverse, precision=HIGHEST,
        preferred_element_type=jnp.float32,
    )
    return (updated_side, head_solution)


def solution(mesh):
    fine = Mesh(mesh.devices.reshape(Z, Y, C, X), ("z", "y", "c", "x"))
    return jax.shard_map(
        on_device,
        mesh=fine,
        in_specs=(P(ROW_AXES, "x"),) * 3,
        out_specs=(P(ROW_AXES, "x"), P(("x",) + ROW_AXES, None)),
        check_vma=False,
    )
```

```python
import jax
import jax.numpy as jnp
from jax import lax
from jax.experimental import pallas as pl
from jax.experimental.pallas import tpu as pltpu
from jax.sharding import Mesh
from jax.sharding import PartitionSpec as P


ROW_AXES = ("z", "y", "c")
Z, Y, C, X = 8, 4, 2, 4
HIGHEST = lax.Precision.HIGHEST
HIGH = lax.Precision.HIGH


def dot(a, b):
    return jnp.dot(a, b, precision=HIGHEST, preferred_element_type=jnp.float32)


def block_inverses(blocks):
    row = lax.broadcasted_iota(jnp.int32, (256, 256), 0)
    lane = lax.broadcasted_iota(jnp.int32, (256, 256), 1)
    i32, lane32 = row[:32], lane[:32]
    j32 = lane32 % 32
    diagonal = row // 32 == lane // 32

    def spread(v):
        return jnp.where(diagonal, jnp.concatenate([v] * 8, axis=0), 0.0)

    packs = []
    for block in blocks:
        p = jnp.zeros((32, 256), jnp.float32)
        for b in range(8):
            p = jnp.where(lane32 // 32 == b, block(b * 32, 32), p)
        packs.append(p)
    ds = [jnp.where(i32 == j32, 1.0 / p, 0.0) for p in packs]
    for s in (1, 2, 4, 8, 16):
        m = (i32 // (2 * s) == j32 // (2 * s)) & (i32 // s != j32 // s) & (i32 > j32)
        eds = [dot(jnp.where(m, p, 0.0), spread(d)) for p, d in zip(packs, ds)]
        ds = [d - dot(d, spread(e)) for d, e in zip(ds, eds)]
    full = [spread(d) for d in ds]
    for n in (32, 64, 128):
        same = row // (2 * n) == lane // (2 * n)
        low = row % (2 * n) >= n
        left = lane % (2 * n) < n
        ln = lane[:n]
        reps = 256 // n
        bs, cs = [], []
        for block, f in zip(blocks, full):
            bp = jnp.zeros((n, 256), jnp.float32)
            cp = jnp.zeros((n, 256), jnp.float32)
            for b in range(reps // 2):
                here = ln // (2 * n) == b
                bp = jnp.where(here & (ln % (2 * n) < n), block(b * 2 * n + n, n), bp)
                cp = jnp.where(here & (ln % (2 * n) >= n), f[b * 2 * n + n : b * 2 * n + 2 * n, :], cp)
            bs.append(bp)
            cs.append(cp)
        bas = [dot(bp, f) for bp, f in zip(bs, full)]
        rs = [
            dot(cp, jnp.where(same & low, jnp.concatenate([ba] * reps, axis=0), 0.0))
            for cp, ba in zip(cs, bas)
        ]
        full = [
            f - jnp.where(same & low & left, jnp.concatenate([r] * reps, axis=0), 0.0)
            for f, r in zip(full, rs)
        ]
    return full


def diagonal_kernel(x_ref, own_ref, out_ref):
    start = pl.multiple_of(x_ref[0] * 256, 256)
    out_ref[...] = own_ref[...]
    (inverse,) = block_inverses([lambda r, n: own_ref[pl.ds(start + r, n), :]])
    out_ref[pl.ds(start, 256), :] = inverse


def load_lower(place_ref, mine_ref, other_ref, lower):
    x = place_ref[0]
    core = place_ref[1]
    near = pl.ds(pl.multiple_of(core * 512, 512), 512)
    far = pl.ds(pl.multiple_of((1 - core) * 512, 512), 512)
    for i, by in enumerate((0, 3, 1, 2)):
        lower[(x + by) % X, near, :] = mine_ref[i]
        lower[(x + by) % X, far, :] = other_ref[i]


def forward_kernel(place_ref, mine_ref, other_ref, side_ref, out_ref, lower):
    load_lower(place_ref, mine_ref, other_ref, lower)
    for b in range(4):
        rows = pl.ds(b * 256, 256)
        value = side_ref[rows, :]
        for k in range(b):
            value = value - dot(lower[k, rows, :], out_ref[pl.ds(k * 256, 256), :])
        out_ref[rows, :] = dot(lower[b, rows, :], value)


def backward_kernel(place_ref, mine_ref, other_ref, target_ref, out_ref, lower):
    load_lower(place_ref, mine_ref, other_ref, lower)
    for b in (3, 2, 1, 0):
        value = target_ref[:, pl.ds(b * 256, 256)]
        for k in range(b + 1, 4):
            value = value - dot(out_ref[:, pl.ds(k * 256, 256)], lower[b, pl.ds(k * 256, 256), :])
        out_ref[:, pl.ds(b * 256, 256)] = dot(value, lower[b, pl.ds(b * 256, 256), :])


SMEM = pl.BlockSpec(memory_space=pltpu.SMEM)
VMEM = pl.BlockSpec(memory_space=pltpu.VMEM)


def call(kernel, shape, place, operands, scratch=()):
    return pl.pallas_call(
        kernel,
        out_shape=jax.ShapeDtypeStruct(shape, jnp.float32),
        in_specs=[SMEM] + [VMEM] * len(operands),
        out_specs=VMEM,
        scratch_shapes=[pltpu.VMEM(s, jnp.float32) for s in scratch],
        compiler_params=pltpu.CompilerParams(vmem_limit_bytes=40 * 1024 * 1024),
    )(place, *operands)


def shift(value, axis, by):
    size = lax.axis_size(axis)
    return lax.ppermute(value, axis, [(i, (i + by) % size) for i in range(size)])


def device(z, y, c):
    return (z * Y + y) * C + c


def tree_steps():
    orders = {
        0: [("z", 4), ("z", 2), ("z", 1), ("y", 2), ("y", 1)],
        1: [("y", 2), ("y", 1), ("z", 4), ("z", 2), ("z", 1)],
    }
    steps = []
    for t in range(5):
        pairs = []
        for core, order in orders.items():
            holders = [(0, 0)]
            for axis, d in order[:t]:
                holders += [(a + d, b) if axis == "z" else (a, b + d) for a, b in holders]
            axis, d = order[t]
            for a, b in holders:
                to = (a + d, b) if axis == "z" else (a, b + d)
                pairs.append((device(a, b, core), device(*to, core)))
        steps.append(pairs)
    return steps


TREE = tree_steps()


def first_halves(array, axis):
    low, high = jnp.split(array, 2, axis=axis)
    other = lax.ppermute(high, ROW_AXES, [(0, 1)])
    return jnp.where(lax.axis_index("c") == 0, low, other)


def spread_step(held, step):
    z, y, c = (lax.axis_index(a) for a in ROW_AXES)
    z_code = z // 4 + 2 * ((z // 2) % 2) + 4 * (z % 2)
    y_code = y // 2 + 2 * (y % 2)
    code = jnp.where(c == 0, z_code + 8 * y_code, y_code + 4 * z_code)
    got = lax.ppermute(held, ROW_AXES, TREE[step])
    return jnp.where(code >> step == 1, got, held)


def join_halves(half):
    core = lax.axis_index("c")
    other = shift(half, "c", 1)
    return jnp.concatenate(
        [jnp.where(core == 0, half, other), jnp.where(core == 0, other, half)], axis=1
    )


def gather_cols(own):
    half = own.shape[0] // 2
    left = shift(own, "x", 1)
    right = shift(own, "x", -1)
    top = shift(left[:half], "x", 1)
    bottom = shift(right[half:], "x", -1)
    return left, right, top, bottom


def rotate(value):
    x = lax.axis_index("x")
    out = jnp.zeros(value.shape, jnp.float32)
    for i, place in enumerate((0, 3, 1, 2)):
        out = lax.dynamic_update_slice(out, value[:, 256 * i : 256 * (i + 1)], (0, ((x + place) % X) * 256))
    return out


def steps(factor, right_side, later_solution):
    x = lax.axis_index("x")
    z, y, c = (lax.axis_index(a) for a in ROW_AXES)
    is_head = lax.axis_index(ROW_AXES) == 0
    place = jnp.stack([x, c])
    left, right, top, bottom = gather_cols(factor)
    own_lower = call(diagonal_kernel, (1024, 256), place, (factor,))
    side = first_halves(right_side, 1)
    low = first_halves(own_lower, 0)
    for t in range(5):
        side = spread_step(side, t)
        low = spread_step(low, t)
    opposite = jnp.concatenate([top, bottom], axis=0)
    factor_blocks = (factor, left, right, opposite)
    partial = [
        lax.dot_general(later_solution, f, (((0,), (0,)), ((), ())), precision=HIGH,
                        preferred_element_type=jnp.float32)
        for f in factor_blocks
    ]
    first = jnp.concatenate(partial[:2], axis=1)
    second = jnp.concatenate(partial[2:], axis=1)
    keep = jnp.where(is_head, 0.0, jnp.where(c == 0, first, second))
    give = jnp.where(is_head, 0.0, jnp.where(c == 0, second, first))
    part = keep + shift(give, "c", 1)
    part = part.reshape(2, 2, 2, 2, 2, 8, 512)
    for axis, index, bit, dim in (("y", y, 1, 4), ("z", z, 1, 2), ("y", y, 2, 3), ("z", z, 2, 1), ("z", z, 4, 0)):
        mine = (index // bit) % 2
        kept = lax.dynamic_slice_in_dim(part, mine, 1, dim)
        sent = lax.dynamic_slice_in_dim(part, 1 - mine, 1, dim)
        size = lax.axis_size(axis)
        part = kept + lax.ppermute(sent, axis, [(i, i ^ bit) for i in range(size)])
    part = part.reshape(8, 512)
    kept = lax.dynamic_slice_in_dim(part, 4 * c, 4, 0)
    sent = lax.dynamic_slice_in_dim(part, 4 * (1 - c), 4, 0)
    other = shift(sent, "c", 1)
    both = jnp.concatenate([jnp.where(c == 0, kept, other), jnp.where(c == 0, other, kept)], axis=1)
    summed = rotate(both)
    low_left, low_right, low_top, low_bottom = gather_cols(low)
    low_mine = jnp.stack([low, low_left, low_right, jnp.concatenate([low_top, low_bottom])])
    low_other = shift(low_mine, "c", 1)
    solved_half = call(
        forward_kernel, (1024, 128), place, (low_mine, low_other, side),
        scratch=[(4, 1024, 256)],
    )
    solved = join_halves(solved_half)
    product = 0.0
    for f, by in zip(factor_blocks, (0, 3, 1, 2)):
        rows = lax.dynamic_slice_in_dim(solved, ((x + by) % X) * 256, 256, 0)
        product = product + jnp.dot(
            f, rows, precision=HIGH, preferred_element_type=jnp.float32
        )
    updated_side = jnp.where(is_head, solved, right_side - product)
    share = lax.axis_index(ROW_AXES) * 4
    pick = (share + jnp.arange(4)[:, None] == jnp.arange(256)[None, :]).astype(jnp.float32)
    solved_share = lax.dot_general(
        pick, solved, (((1,), (1,)), ((), ())), precision=HIGHEST,
        preferred_element_type=jnp.float32,
    )
    head_solution = call(
        backward_kernel, (4, 1024), place,
        (low_mine, low_other, solved_share - summed), scratch=[(4, 1024, 256)],
    )
    return (updated_side, head_solution)


def solution(mesh):
    fine = Mesh(mesh.devices.reshape(Z, Y, C, X), ("z", "y", "c", "x"))
    return jax.shard_map(
        steps,
        mesh=fine,
        in_specs=(P(ROW_AXES, "x"),) * 3,
        out_specs=(P(ROW_AXES, "x"), P(("x",) + ROW_AXES, None)),
        check_vma=False,
    )
```

```python
import jax
import jax.numpy as jnp
from jax import lax
from jax.experimental import pallas as pl
from jax.experimental.pallas import tpu as pltpu
from jax.sharding import Mesh
from jax.sharding import PartitionSpec as P


ROW_AXES = ("z", "y", "c")
Z, Y, C, X = 8, 4, 2, 4
HIGHEST = lax.Precision.HIGHEST
HIGH = lax.Precision.HIGH


def dot(a, b):
    return jnp.dot(a, b, precision=HIGHEST, preferred_element_type=jnp.float32)


def block_inverses(blocks):
    row = lax.broadcasted_iota(jnp.int32, (256, 256), 0)
    lane = lax.broadcasted_iota(jnp.int32, (256, 256), 1)
    i32, lane32 = row[:32], lane[:32]
    j32 = lane32 % 32
    diagonal = row // 32 == lane // 32

    def spread(v):
        return jnp.where(diagonal, jnp.concatenate([v] * 8, axis=0), 0.0)

    packs = []
    for block in blocks:
        p = jnp.zeros((32, 256), jnp.float32)
        for b in range(8):
            p = jnp.where(lane32 // 32 == b, block(b * 32, 32), p)
        packs.append(p)
    ds = [jnp.where(i32 == j32, 1.0 / p, 0.0) for p in packs]
    for s in (1, 2, 4, 8, 16):
        m = (i32 // (2 * s) == j32 // (2 * s)) & (i32 // s != j32 // s) & (i32 > j32)
        eds = [dot(jnp.where(m, p, 0.0), spread(d)) for p, d in zip(packs, ds)]
        ds = [d - dot(d, spread(e)) for d, e in zip(ds, eds)]
    full = [spread(d) for d in ds]
    for n in (32, 64, 128):
        same = row // (2 * n) == lane // (2 * n)
        low = row % (2 * n) >= n
        left = lane % (2 * n) < n
        ln = lane[:n]
        reps = 256 // n
        bs, cs = [], []
        for block, f in zip(blocks, full):
            bp = jnp.zeros((n, 256), jnp.float32)
            cp = jnp.zeros((n, 256), jnp.float32)
            for b in range(reps // 2):
                here = ln // (2 * n) == b
                bp = jnp.where(here & (ln % (2 * n) < n), block(b * 2 * n + n, n), bp)
                cp = jnp.where(here & (ln % (2 * n) >= n), f[b * 2 * n + n : b * 2 * n + 2 * n, :], cp)
            bs.append(bp)
            cs.append(cp)
        bas = [dot(bp, f) for bp, f in zip(bs, full)]
        rs = [
            dot(cp, jnp.where(same & low, jnp.concatenate([ba] * reps, axis=0), 0.0))
            for cp, ba in zip(cs, bas)
        ]
        full = [
            f - jnp.where(same & low & left, jnp.concatenate([r] * reps, axis=0), 0.0)
            for f, r in zip(full, rs)
        ]
    return full


def diagonal_kernel(x_ref, own_ref, out_ref):
    start = pl.multiple_of(x_ref[0] * 256, 256)
    out_ref[...] = own_ref[...]
    (inverse,) = block_inverses([lambda r, n: own_ref[pl.ds(start + r, n), :]])
    out_ref[pl.ds(start, 256), :] = inverse


def load_lower(place_ref, mine_ref, other_ref, lower):
    x = place_ref[0]
    core = place_ref[1]
    near = pl.ds(pl.multiple_of(core * 512, 512), 512)
    far = pl.ds(pl.multiple_of((1 - core) * 512, 512), 512)
    for i, by in enumerate((0, 3, 1, 2)):
        lower[(x + by) % X, near, :] = mine_ref[i]
        lower[(x + by) % X, far, :] = other_ref[i]


def forward_kernel(place_ref, mine_ref, other_ref, side_ref, out_ref, lower):
    load_lower(place_ref, mine_ref, other_ref, lower)
    for b in range(4):
        rows = pl.ds(b * 256, 256)
        value = side_ref[rows, :]
        for k in range(b):
            value = value - dot(lower[k, rows, :], out_ref[pl.ds(k * 256, 256), :])
        out_ref[rows, :] = dot(lower[b, rows, :], value)


def backward_kernel(place_ref, mine_ref, other_ref, target_ref, out_ref, lower):
    load_lower(place_ref, mine_ref, other_ref, lower)
    for b in (3, 2, 1, 0):
        value = target_ref[:, pl.ds(b * 256, 256)]
        for k in range(b + 1, 4):
            value = value - dot(out_ref[:, pl.ds(k * 256, 256)], lower[b, pl.ds(k * 256, 256), :])
        out_ref[:, pl.ds(b * 256, 256)] = dot(value, lower[b, pl.ds(b * 256, 256), :])


SMEM = pl.BlockSpec(memory_space=pltpu.SMEM)
VMEM = pl.BlockSpec(memory_space=pltpu.VMEM)


def call(kernel, shape, place, operands, scratch=()):
    return pl.pallas_call(
        kernel,
        out_shape=jax.ShapeDtypeStruct(shape, jnp.float32),
        in_specs=[SMEM] + [VMEM] * len(operands),
        out_specs=VMEM,
        scratch_shapes=[pltpu.VMEM(s, jnp.float32) for s in scratch],
        compiler_params=pltpu.CompilerParams(vmem_limit_bytes=40 * 1024 * 1024),
    )(place, *operands)


def shift(value, axis, by):
    size = lax.axis_size(axis)
    return lax.ppermute(value, axis, [(i, (i + by) % size) for i in range(size)])


def device(z, y, c):
    return (z * Y + y) * C + c


Z_TREE = (((0, 3),), ((0, 6), (3, 5)), ((0, 1), (3, 2), (5, 4), (6, 7)))
Y_TREE = (((0, 1),), ((0, 3), (1, 2)))


def tree_steps(sign):
    steps = []
    for t in range(5):
        pairs = []
        for a, b in Z_TREE[t] if t < 3 else ():
            pairs.append((device(sign * a % Z, 0, 0), device(sign * b % Z, 0, 0)))
        for a, b in Y_TREE[t - 3] if t >= 3 else ():
            for z in range(Z):
                pairs.append((device(z, sign * a % Y, 0), device(z, sign * b % Y, 0)))
        for a, b in Y_TREE[t] if t < 2 else ():
            pairs.append((device(0, sign * a % Y, 1), device(0, sign * b % Y, 1)))
        for a, b in Z_TREE[t - 2] if t >= 2 else ():
            for y in range(Y):
                pairs.append((device(sign * a % Z, y, 1), device(sign * b % Z, y, 1)))
        steps.append(pairs)
    return steps


TREE = {1: tree_steps(1), -1: tree_steps(-1)}


def first_halves(array, axis):
    low, high = jnp.split(array, 2, axis=axis)
    other = lax.ppermute(high, ROW_AXES, [(0, 1)])
    return jnp.where(lax.axis_index("c") == 0, low, other)


def arrival(sign):
    z, y, c = (lax.axis_index(a) for a in ROW_AXES)
    z = (sign * z) % Z
    y = (sign * y) % Y
    by_z = jnp.where(z == 3, 0, jnp.where((z == 5) | (z == 6), 1, jnp.where(z == 0, -9, 2)))
    by_y = jnp.where(y == 1, 0, jnp.where(y == 0, -9, 1))
    return jnp.where(
        c == 0, jnp.where(y == 0, by_z, 3 + by_y), jnp.where(z == 0, by_y, 2 + by_z)
    )


def spread_step(held, step, sign):
    got = lax.ppermute(held, ROW_AXES, TREE[sign][step])
    return jnp.where(arrival(sign) == step, got, held)


def join_halves(half):
    core = lax.axis_index("c")
    other = shift(half, "c", 1)
    return jnp.concatenate(
        [jnp.where(core == 0, half, other), jnp.where(core == 0, other, half)], axis=1
    )


def gather_cols(own):
    half = own.shape[0] // 2
    left = shift(own, "x", 1)
    right = shift(own, "x", -1)
    top = shift(left[:half], "x", 1)
    bottom = shift(right[half:], "x", -1)
    return left, right, top, bottom


def rotate(value):
    x = lax.axis_index("x")
    out = jnp.zeros(value.shape, jnp.float32)
    for i, place in enumerate((0, 3, 1, 2)):
        out = lax.dynamic_update_slice(out, value[:, 256 * i : 256 * (i + 1)], (0, ((x + place) % X) * 256))
    return out


def steps(factor, right_side, later_solution):
    x = lax.axis_index("x")
    z, y, c = (lax.axis_index(a) for a in ROW_AXES)
    is_head = lax.axis_index(ROW_AXES) == 0
    place = jnp.stack([x, c])
    left, right, top, bottom = gather_cols(factor)
    own_lower = call(diagonal_kernel, (1024, 256), place, (factor,))
    side = first_halves(right_side, 1)
    low = first_halves(own_lower, 0)
    for t in range(5):
        side = spread_step(side, t, -1)
        low = spread_step(low, t, 1)
    opposite = jnp.concatenate([top, bottom], axis=0)
    factor_blocks = (factor, left, right, opposite)
    partial = [
        lax.dot_general(later_solution, f, (((0,), (0,)), ((), ())), precision=HIGH,
                        preferred_element_type=jnp.float32)
        for f in factor_blocks
    ]
    first = jnp.concatenate(partial[:2], axis=1)
    second = jnp.concatenate(partial[2:], axis=1)
    keep = jnp.where(is_head, 0.0, jnp.where(c == 0, first, second))
    give = jnp.where(is_head, 0.0, jnp.where(c == 0, second, first))
    part = keep + shift(give, "c", 1)
    part = part.reshape(2, 2, 2, 2, 2, 8, 512)
    for axis, index, bit, dim in (("y", y, 1, 4), ("z", z, 1, 2), ("y", y, 2, 3), ("z", z, 2, 1), ("z", z, 4, 0)):
        mine = (index // bit) % 2
        kept = lax.dynamic_slice_in_dim(part, mine, 1, dim)
        sent = lax.dynamic_slice_in_dim(part, 1 - mine, 1, dim)
        size = lax.axis_size(axis)
        part = kept + lax.ppermute(sent, axis, [(i, i ^ bit) for i in range(size)])
    part = part.reshape(8, 512)
    kept = lax.dynamic_slice_in_dim(part, 4 * c, 4, 0)
    sent = lax.dynamic_slice_in_dim(part, 4 * (1 - c), 4, 0)
    other = shift(sent, "c", 1)
    both = jnp.concatenate([jnp.where(c == 0, kept, other), jnp.where(c == 0, other, kept)], axis=1)
    summed = rotate(both)
    low_left, low_right, low_top, low_bottom = gather_cols(low)
    low_mine = jnp.stack([low, low_left, low_right, jnp.concatenate([low_top, low_bottom])])
    low_other = shift(low_mine, "c", 1)
    solved_half = call(
        forward_kernel, (1024, 128), place, (low_mine, low_other, side),
        scratch=[(4, 1024, 256)],
    )
    solved = join_halves(solved_half)
    product = 0.0
    for f, by in zip(factor_blocks, (0, 3, 1, 2)):
        rows = lax.dynamic_slice_in_dim(solved, ((x + by) % X) * 256, 256, 0)
        product = product + jnp.dot(
            f, rows, precision=HIGH, preferred_element_type=jnp.float32
        )
    updated_side = jnp.where(is_head, solved, right_side - product)
    share = lax.axis_index(ROW_AXES) * 4
    pick = (share + jnp.arange(4)[:, None] == jnp.arange(256)[None, :]).astype(jnp.float32)
    solved_share = lax.dot_general(
        pick, solved, (((1,), (1,)), ((), ())), precision=HIGHEST,
        preferred_element_type=jnp.float32,
    )
    head_solution = call(
        backward_kernel, (4, 1024), place,
        (low_mine, low_other, solved_share - summed), scratch=[(4, 1024, 256)],
    )
    return (updated_side, head_solution)


def solution(mesh):
    fine = Mesh(mesh.devices.reshape(Z, Y, C, X), ("z", "y", "c", "x"))
    return jax.shard_map(
        steps,
        mesh=fine,
        in_specs=(P(ROW_AXES, "x"),) * 3,
        out_specs=(P(ROW_AXES, "x"), P(("x",) + ROW_AXES, None)),
        check_vma=False,
    )
```
